32 devices in a mesh: seq: 16 (over z, y, x), rep: 2 (over core).
Axes of the slice: x: 2, y: 2, z: 4, core: 2. Of those that a mesh axis runs over, the one named last changes fastest.
Arguments:
- tokens: bfloat16 [4, 48, 180, 768], P('rep', 'seq'), may hold values from -6 to 6
- cotangent: bfloat16 [4, 48, 180, 768], P('rep', 'seq'), may hold values from -6 to 6
- in_weight: bfloat16 [2, 8, 96, 96], replicated, may hold values from -0.21875 to 0.21875
- in_bias: float32 [2, 768], replicated, may hold values from -0.6 to 0.6
- out_weight: bfloat16 [2, 8, 96, 96], replicated, may hold values from -0.21875 to 0.21875
- out_bias: float32 [2, 768], replicated, may hold values from -0.12 to 0.12
Outputs:
- mixed_out: bfloat16 [4, 48, 180, 768], P('rep', 'seq')
- tokens_grad: bfloat16 [4, 48, 180, 768], P('rep', 'seq')
- in_weight_grad: float32 [2, 8, 96, 96], replicated
- in_bias_grad: float32 [2, 768], replicated
- out_weight_grad: float32 [2, 8, 96, 96], replicated
- out_bias_grad: float32 [2, 768], replicated
The draws below stay inside these ranges and needn't reach their ends.
All inputs are finite; a program needn't handle non-finite values.
Results may differ from the reference program's by a relative error of at most 0.0094.
Values may be sent and summed in bfloat16 or wider, within the bound.
A program may use at most 64 MiB of HBM per device.

```python
import math
import jax
import jax.numpy as jnp
from jax import lax

D = 768
BLOCKS = 8
BLOCK = 96
COLS = 180
MODES = 64
ROWS = 48
BATCH = 4


def shard_levels(key, extent, cuts, low, largest):
    def one(axis_at, shards_of):
        heights = jax.random.uniform(jax.random.fold_in(jax.random.fold_in(key, 6), axis_at), (shards_of,), jnp.float32, low / len(cuts), largest / len(cuts))
        return jnp.repeat(jnp.exp(heights), extent[axis_at] // shards_of).reshape((-1,) + (1,) * (len(extent) - axis_at - 1))

    factor_of = one(*cuts[0])
    for cut in cuts[1:]:
        factor_of = factor_of * one(*cut)
    return factor_of


def scatter_about(key, dims, width, limit, pieces=(), kind=jnp.bfloat16):
    drawn = width * jax.random.normal(key, dims, jnp.float32)
    if pieces:
        drawn = drawn * shard_levels(key, dims, pieces, -0.22, 0.18)
    return jnp.clip(drawn, -limit, limit).astype(kind)


def setup_inputs(seed: int = 0) -> dict:
    splits = jax.random.split(jax.random.key(seed), 7)
    tokens = scatter_about(splits[0], (BATCH, ROWS, COLS, D), 1.0, 6.0, ((0, 2), (1, 16)))
    cotangent = scatter_about(splits[1], (BATCH, ROWS, COLS, D), 1.0, 6.0, ((0, 2), (1, 16)))
    in_weight = scatter_about(splits[2], (2, BLOCKS, BLOCK, BLOCK), (8 * BLOCK) ** -0.5, 0.21875)
    in_bias = scatter_about(splits[3], (2, D), 0.1, 0.6, (), jnp.float32)
    out_weight = scatter_about(splits[4], (2, BLOCKS, BLOCK, BLOCK), (8 * BLOCK) ** -0.5, 0.21875)
    out_bias = scatter_about(splits[5], (2, D), 0.02, 0.12, (), jnp.float32)
    return {"tokens": tokens, "cotangent": cotangent, "in_weight": in_weight, "in_bias": in_bias, "out_weight": out_weight, "out_bias": out_bias}


def widen(operand):
    return operand.astype(jnp.float32)

def grid_tables(length, modes):
    position = jnp.arange(length, dtype=jnp.int32)
    frequency = jnp.arange(modes, dtype=jnp.int32)
    residue = position[:, None] * frequency[None, :] % length
    angles = residue.astype(jnp.float32) * (2.0 * math.pi / length)
    factor = 1.0 / math.sqrt(length)
    cosine_table = (jnp.cos(angles) * factor).astype(jnp.bfloat16)
    sine_table = (jnp.sin(angles) * factor).astype(jnp.bfloat16)
    return (cosine_table, sine_table)

def column_tables(grid_width, modes):
    cosine_table, sine_table = grid_tables(grid_width, modes)
    forward = jnp.stack([cosine_table, -sine_table], axis=2)
    doubling = jnp.where(jnp.arange(modes) == 0, 1.0, 2.0).astype(jnp.bfloat16)[:, None]
    inverse = jnp.stack([cosine_table.T * doubling, -(sine_table.T * doubling)], axis=1)
    return (forward, inverse)

def row_table(length):
    cosine_table, sine_table = grid_tables(length, length)
    upper_rows = jnp.stack([cosine_table, sine_table], axis=2)
    lower_rows = jnp.stack([-sine_table, cosine_table], axis=2)
    return jnp.stack([upper_rows, lower_rows], axis=1)

def block_weights(weight):
    real_part, imag_part = (weight[0], weight[1])
    upper_half = jnp.stack([real_part, imag_part], axis=2)
    lower_half = jnp.stack([-imag_part, real_part], axis=2)
    return jnp.stack([upper_half, lower_half], axis=1)

def fold_blocks(blockwise):
    real_part = blockwise[:, 0, :, 0, :] + blockwise[:, 1, :, 1, :]
    imag_part = blockwise[:, 0, :, 1, :] - blockwise[:, 1, :, 0, :]
    return jnp.stack([real_part, imag_part])

def reference(tokens, cotangent, in_weight, in_bias, out_weight, out_bias):
    column_forward, column_inverse = column_tables(COLS, MODES)
    row_matrix = row_table(ROWS)
    weights_in = block_weights(in_weight)
    weights_out = block_weights(out_weight)
    bias_in = in_bias.reshape(2, BLOCKS, BLOCK)
    bias_out = out_bias.reshape(2, BLOCKS, BLOCK)
    mode_count = ROWS * MODES

    def one_sample(pair):
        sample_tokens, sample_cotangent = pair
        spec_rows = jnp.einsum('hwd,wkc->hkcd', widen(sample_tokens), widen(column_forward)).astype(jnp.bfloat16)
        spectrum = jnp.einsum('qehc,hkcd->qked', widen(row_matrix), widen(spec_rows)).astype(jnp.bfloat16)
        flat_modes = spectrum.reshape(mode_count, 2, BLOCKS, BLOCK)
        hidden_pre = jnp.einsum('mcbi,bciej->mebj', widen(flat_modes), widen(weights_in)) + bias_in
        hidden = jax.nn.gelu(hidden_pre).astype(jnp.bfloat16)
        spectrum_out = (jnp.einsum('mcbi,bciej->mebj', widen(hidden), widen(weights_out)) + bias_out).astype(jnp.bfloat16)
        back_rows = jnp.einsum('qehc,qked->hkcd', widen(row_matrix), widen(spectrum_out.reshape(ROWS, MODES, 2, D))).astype(jnp.bfloat16)
        mixed = (widen(sample_tokens) + jnp.einsum('hkcd,kcw->hwd', widen(back_rows), widen(column_inverse))).astype(jnp.bfloat16)
        cot_rows = jnp.einsum('hwd,kcw->hkcd', widen(sample_cotangent), widen(column_inverse)).astype(jnp.bfloat16)
        incoming = jnp.einsum('qehc,hkcd->qked', widen(row_matrix), widen(cot_rows)).astype(jnp.bfloat16)
        incoming = incoming.reshape(mode_count, 2, BLOCKS, BLOCK)
        out_bias_part = lax.optimization_barrier(jnp.sum(widen(incoming), axis=0)).reshape(2, D)
        out_weight_part = fold_blocks(jnp.einsum('mcbi,mebj->bciej', widen(hidden), widen(incoming)))
        hidden_grad = jnp.einsum('mebj,bciej->mcbi', widen(incoming), widen(weights_out))
        pre_grad = jax.vjp(jax.nn.gelu, hidden_pre)[1](hidden_grad)[0].astype(jnp.bfloat16)
        in_bias_part = lax.optimization_barrier(jnp.sum(widen(pre_grad), axis=0)).reshape(2, D)
        in_weight_part = fold_blocks(jnp.einsum('mcbi,mebj->bciej', widen(flat_modes), widen(pre_grad)))
        spectrum_grad = jnp.einsum('mebj,bciej->mcbi', widen(pre_grad), widen(weights_in)).astype(jnp.bfloat16)
        rows_grad = jnp.einsum('qehc,qked->hkcd', widen(row_matrix), widen(spectrum_grad.reshape(ROWS, MODES, 2, D))).astype(jnp.bfloat16)
        grad_tokens = (widen(sample_cotangent) + jnp.einsum('hkcd,wkc->hwd', widen(rows_grad), widen(column_forward))).astype(jnp.bfloat16)
        return (mixed, grad_tokens, in_weight_part, in_bias_part, out_weight_part, out_bias_part)
    outcome = lax.map(one_sample, (tokens, cotangent))
    return (outcome[0], outcome[1], lax.optimization_barrier(jnp.sum(outcome[2], axis=0)) / BATCH, lax.optimization_barrier(jnp.sum(outcome[3], axis=0)) / BATCH, lax.optimization_barrier(jnp.sum(outcome[4], axis=0)) / BATCH, lax.optimization_barrier(jnp.sum(outcome[5], axis=0)) / BATCH)
```

```python
import functools
import math

import jax
import jax.numpy as jnp
import ml_dtypes
import numpy as np
from jax import lax
from jax.experimental import pallas as pl
from jax.experimental.pallas import tpu as pltpu
from jax.sharding import PartitionSpec as P

BLOCKS = 8
BLOCK = 96
MODES = 64


def grid_tables(length, modes):
    position = jnp.arange(length, dtype=jnp.int32)
    frequency = jnp.arange(modes, dtype=jnp.int32)
    residue = position[:, None] * frequency[None, :] % length
    angles = residue.astype(jnp.float32) * (2.0 * math.pi / length)
    factor = 1.0 / math.sqrt(length)
    cosine_table = (jnp.cos(angles) * factor).astype(jnp.bfloat16)
    sine_table = (jnp.sin(angles) * factor).astype(jnp.bfloat16)
    return (cosine_table, sine_table)


def column_tables(grid_width, modes):
    cosine_table, sine_table = grid_tables(grid_width, modes)
    forward = jnp.stack([cosine_table, -sine_table], axis=2)
    doubling = jnp.where(jnp.arange(modes) == 0, 1.0, 2.0).astype(jnp.bfloat16)[:, None]
    inverse = jnp.stack([cosine_table.T * doubling, -(sine_table.T * doubling)], axis=1)
    return (forward, inverse)


def row_table(length):
    cosine_table, sine_table = grid_tables(length, length)
    upper_rows = jnp.stack([cosine_table, sine_table], axis=2)
    lower_rows = jnp.stack([-sine_table, cosine_table], axis=2)
    return jnp.stack([upper_rows, lower_rows], axis=1)


def block_weights(weight):
    real_part, imag_part = (weight[0], weight[1])
    upper_half = jnp.stack([real_part, imag_part], axis=2)
    lower_half = jnp.stack([-imag_part, real_part], axis=2)
    return jnp.stack([upper_half, lower_half], axis=1)


def fold_blocks(blockwise):
    real_part = blockwise[:, 0, :, 0, :] + blockwise[:, 1, :, 1, :]
    imag_part = blockwise[:, 0, :, 1, :] - blockwise[:, 1, :, 0, :]
    return jnp.stack([real_part, imag_part])


def mix_forward(spectrum, weights_in, weights_out, bias_in, bias_out):
    mode_count = spectrum.shape[0] * spectrum.shape[1] * spectrum.shape[2]
    flat_modes = spectrum.reshape(mode_count, 2, BLOCKS, BLOCK)
    hidden_pre = (
        jnp.einsum("mcbi,bciej->mebj", flat_modes, weights_in, preferred_element_type=jnp.float32)
        + bias_in
    )
    hidden = jax.nn.gelu(hidden_pre).astype(jnp.bfloat16)
    spectrum_out = (
        jnp.einsum("mcbi,bciej->mebj", hidden, weights_out, preferred_element_type=jnp.float32)
        + bias_out
    )
    return (
        flat_modes,
        hidden_pre,
        hidden,
        spectrum_out.astype(jnp.bfloat16).reshape(spectrum.shape),
    )


def mix_backward(flat_modes, hidden_pre, hidden, incoming, weights_in, weights_out):
    incoming_flat = incoming.reshape(flat_modes.shape)
    out_bias_part = jnp.sum(incoming_flat.astype(jnp.float32), axis=0).reshape(2, -1)
    out_weight_part = fold_blocks(
        jnp.einsum("mcbi,mebj->bciej", hidden, incoming_flat, preferred_element_type=jnp.float32)
    )
    hidden_grad = jnp.einsum(
        "mebj,bciej->mcbi", incoming_flat, weights_out, preferred_element_type=jnp.float32
    )
    pre_grad = jax.vjp(jax.nn.gelu, hidden_pre)[1](hidden_grad)[0].astype(jnp.bfloat16)
    in_bias_part = jnp.sum(pre_grad.astype(jnp.float32), axis=0).reshape(2, -1)
    in_weight_part = fold_blocks(
        jnp.einsum("mcbi,mebj->bciej", flat_modes, pre_grad, preferred_element_type=jnp.float32)
    )
    spectrum_grad = jnp.einsum(
        "mebj,bciej->mcbi", pre_grad, weights_in, preferred_element_type=jnp.float32
    )
    spectrum_grad = spectrum_grad.astype(jnp.bfloat16).reshape(incoming.shape)
    return (spectrum_grad, (in_weight_part, in_bias_part, out_weight_part, out_bias_part))


def shards_plain(tokens, cotangent, in_weight, in_bias, out_weight, out_bias):
    samples, row_count, grid_width, channels = tokens.shape
    length = row_count * lax.axis_size("seq")
    column_forward, column_inverse = column_tables(grid_width, MODES)
    row_matrix = row_table(length)
    weights_in = block_weights(in_weight)
    weights_out = block_weights(out_weight)
    bias_in = in_bias.reshape(2, BLOCKS, BLOCK)
    bias_out = out_bias.reshape(2, BLOCKS, BLOCK)

    def along_rows(section):
        return jnp.einsum(
            "qehc,shkcd->sqked", row_matrix, section, preferred_element_type=jnp.float32
        ).astype(jnp.bfloat16)

    def back_rows(section):
        return jnp.einsum(
            "qehc,sqked->shkcd", row_matrix, section, preferred_element_type=jnp.float32
        ).astype(jnp.bfloat16)

    spec_rows = jnp.einsum(
        "shwd,wkc->shkcd", tokens, column_forward, preferred_element_type=jnp.float32
    ).astype(jnp.bfloat16)
    spectrum = along_rows(lax.all_to_all(spec_rows, "seq", split_axis=2, concat_axis=1, tiled=True))
    flat_modes, hidden_pre, hidden, spectrum_out = mix_forward(
        spectrum, weights_in, weights_out, bias_in, bias_out
    )
    mixed_grid = jnp.einsum(
        "shkcd,kcw->shwd",
        lax.all_to_all(back_rows(spectrum_out), "seq", split_axis=1, concat_axis=2, tiled=True),
        column_inverse,
        preferred_element_type=jnp.float32,
    )
    cot_rows = jnp.einsum(
        "shwd,kcw->shkcd", cotangent, column_inverse, preferred_element_type=jnp.float32
    ).astype(jnp.bfloat16)
    incoming = along_rows(lax.all_to_all(cot_rows, "seq", split_axis=2, concat_axis=1, tiled=True))
    spectrum_grad, partials = mix_backward(
        flat_modes, hidden_pre, hidden, incoming, weights_in, weights_out
    )
    adjoint_part = jnp.einsum(
        "shkcd,wkc->shwd",
        lax.all_to_all(back_rows(spectrum_grad), "seq", split_axis=1, concat_axis=2, tiled=True),
        column_forward,
        preferred_element_type=jnp.float32,
    )
    mixed_out = (tokens.astype(jnp.float32) + mixed_grid).astype(jnp.bfloat16)
    tokens_grad = (cotangent.astype(jnp.float32) + adjoint_part).astype(jnp.bfloat16)
    totals = lax.psum((partials[0], partials[1], partials[2], partials[3]), ("seq", "rep"))
    divisor = float(samples * lax.axis_size("rep"))
    return (
        mixed_out,
        tokens_grad,
        totals[0] / divisor,
        totals[1] / divisor,
        totals[2] / divisor,
        totals[3] / divisor,
    )


GROUP = math.lcm(BLOCK, 128)
PER_GROUP = GROUP // BLOCK
COPY_A, COPY_B, COPY_C, COPY_D, COPY_E, COPY_F = range(6)
MESH_ID = pl.DeviceIdType.MESH


def host_tables(length, modes):
    residue = np.arange(length)[:, None] * np.arange(modes)[None, :] % length
    angles = residue.astype(np.float32) * np.float32(2.0 * math.pi / length)
    factor = np.float32(1.0 / math.sqrt(length))
    rounded = [(f(angles) * factor).astype(ml_dtypes.bfloat16) for f in (np.cos, np.sin)]
    return [table.astype(np.float32) for table in rounded]


def kernel_tables(width, length, n, samples, rows):
    local = MODES // n
    cosine, sine = host_tables(width, MODES)
    forward = np.stack([cosine.T, -sine.T], axis=1)
    doubled = forward * np.where(np.arange(MODES) == 0, 1.0, 2.0)[:, None, None]
    padded = -(-width // 16) * 16

    def inverse(table):
        table = table.reshape(n, local, 2, width)
        whole = np.zeros((samples, padded, n, samples, local, 2), np.float32)
        for s in range(samples):
            whole[s, :width, :, s] = table.transpose(3, 0, 1, 2)
        return whole.reshape(samples * padded, n * samples * local * 2)

    cosine, sine = host_tables(length, length)
    upper = np.stack([cosine, sine], axis=2)
    lower = np.stack([-sine, cosine], axis=2)
    turn = np.stack([upper, lower], axis=0)
    both = samples * local
    mixing = np.zeros((2, both, length, length, both, 2), np.float32)
    for x in range(both):
        mixing[:, x, :, :, x, :] = turn
    mixing = mixing.reshape(2 * both * length, length * both * 2)

    per = 4 * BLOCK // (2 * n)
    picks = np.zeros((2, n, 16, 4 * BLOCK + 16), np.float32)
    for r in range(2):
        for p in range(n):
            for i in range(16):
                column = (r * n + p) * per + i if i < per else 4 * BLOCK + i - per
                if i < per + 4:
                    picks[r, p, i, column] = 1.0
    flat = [
        forward.reshape(2 * MODES, width),
        doubled.reshape(2 * MODES, width),
        inverse(doubled),
        inverse(forward),
        mixing,
        mixing.T,
        picks.reshape(2 * n * 16, 4 * BLOCK + 16),
    ]
    return [np.ascontiguousarray(t).astype(ml_dtypes.bfloat16) for t in flat]


def dot(a, b, contract=(1, 0)):
    return lax.dot_general(
        a, b, (((contract[0],), (contract[1],)), ((), ())), preferred_element_type=jnp.float32
    )


def mixer(
    n,
    divisor,
    tok,
    cot,
    col_tok,
    col_cot,
    inv_mix,
    inv_grad,
    turn,
    turn_back,
    picks,
    in_weight,
    in_bias,
    out_weight,
    out_bias,
    mixed,
    grad,
    weight_out,
    bias_out,
    send_a,
    send_b,
    send_c,
    send_d,
    send_e,
    recv_a,
    recv_b,
    recv_c,
    recv_d,
    recv_e,
    wide,
    spec,
    hid,
    slope,
    inc,
    pre,
    mixed_modes,
    grads,
    halves,
    half_in,
    part,
    gathered,
    other,
    send_sem,
    recv_sem,
    pair_send,
    pair_recv,
):
    me = lax.axis_index("seq")
    core = lax.axis_index("rep")
    partner = 1 - core
    samples, rows, width, channels = tok.shape
    groups = channels // GROUP
    padded = inv_mix.shape[0] // samples
    chunk = send_a.shape[1]
    row_chunk = chunk // rows
    bf16 = jnp.bfloat16

    barrier = pltpu.get_barrier_semaphore()

    def greet(j, carry):
        peer = lax.rem(me + j, n)
        pl.semaphore_signal(barrier, inc=1, device_id={"seq": peer}, device_id_type=MESH_ID)
        return carry

    lax.fori_loop(1, n, greet, 0)
    pl.semaphore_signal(barrier, inc=1, device_id={"rep": partner}, device_id_type=MESH_ID)

    def to_peer(phase, source, target, j):
        peer = lax.rem(me + j, n)
        return pltpu.make_async_remote_copy(
            src_ref=source(peer),
            dst_ref=target.at[me],
            send_sem=send_sem.at[phase, peer],
            recv_sem=recv_sem.at[phase, me],
            device_id={"seq": peer},
            device_id_type=MESH_ID,
        )

    def from_peer(phase, target, j):
        peer = lax.rem(me + j, n)
        return pltpu.make_async_remote_copy(
            src_ref=target.at[peer],
            dst_ref=target.at[peer],
            send_sem=send_sem.at[phase, peer],
            recv_sem=recv_sem.at[phase, peer],
            device_id={"seq": peer},
            device_id_type=MESH_ID,
        )

    def each(act):
        def step(j, carry):
            act(j)
            return carry

        lax.fori_loop(1, n, step, 0)

    def start(phase, source, target):
        each(lambda j: to_peer(phase, lambda peer: source.at[peer], target, j).start())

    def arrive(phase, target):
        each(lambda j: from_peer(phase, target, j).wait_recv())

    def drain(phase, source, target):
        each(lambda j: to_peer(phase, lambda peer: source.at[peer], target, j).wait_send())

    def columns(tokens, table, send):
        for h in range(rows):
            parts = [
                dot(table[...], tokens[s, h]).reshape(n, row_chunk // samples, channels)
                for s in range(samples)
            ]
            send[:, h * row_chunk : (h + 1) * row_chunk, :] = jnp.concatenate(
                parts, axis=1
            ).astype(bf16)

    columns(tok, col_tok, send_a)
    pl.semaphore_wait(barrier, n)
    start(COPY_A, send_a, recv_a)
    columns(cot, col_cot, send_b)
    start(COPY_B, send_b, recv_b)
    recv_a[me] = send_a[me]
    recv_b[me] = send_b[me]

    row_at = lax.broadcasted_iota(jnp.int32, (BLOCK, GROUP), 0)
    lane_at = lax.broadcasted_iota(jnp.int32, (BLOCK, GROUP), 1)
    for at, weight in enumerate((in_weight, out_weight)):
        for i in range(PER_GROUP):
            place = (lane_at == row_at + i * BLOCK).astype(bf16)
            for c in range(2):
                for g in range(groups):
                    wide[2 * at + c, g, i * BLOCK : (i + 1) * BLOCK, :] = dot(
                        weight[c, g * PER_GROUP + i], place
                    ).astype(bf16)

    half = turn.shape[0] // 2
    scale = math.sqrt(2.0 / math.pi)

    def lanes(g):
        return pl.ds(pl.multiple_of(g * GROUP, GROUP), GROUP)

    def per_group(act):
        def step(g, carry):
            act(g, lanes(g))
            return carry

        lax.fori_loop(0, groups, step, 0)

    def along_rows(recv, at, keep, g):
        keep[g] = dot(turn[...], recv[:, :, at].reshape(turn.shape[1], GROUP)).astype(bf16)

    def back_rows(send, at):
        send[:, :, at] = (
            dot(turn_back[...], mixed_modes[...]).astype(bf16).reshape(n, chunk, GROUP)
        )

    def forward_group(g, at):
        along_rows(recv_a, at, spec, g)
        re, im = spec[g, :half], spec[g, half:]
        w_re, w_im = wide[0, g], wide[1, g]
        for c in range(2):
            if c == 0:
                value = dot(re, w_re) - dot(im, w_im)
            else:
                value = dot(re, w_im) + dot(im, w_re)
            value = value + in_bias[c : c + 1, at]
            square = value * value
            tanh = jnp.tanh(scale * value * (1.0 + 0.044715 * square))
            hid[g, c * half : (c + 1) * half] = (0.5 * value * (1.0 + tanh)).astype(bf16)
            slope[g, c * half : (c + 1) * half] = 0.5 * (1.0 + tanh) + 0.5 * value * (
                1.0 - tanh * tanh
            ) * (scale * (1.0 + (3.0 * 0.044715) * square))
        re, im = hid[g, :half], hid[g, half:]
        w_re, w_im = wide[2, g], wide[3, g]
        mixed_modes[:half] = (
            dot(re, w_re) - dot(im, w_im) + out_bias[0:1, at]
        ).astype(bf16)
        mixed_modes[half:] = (
            dot(re, w_im) + dot(im, w_re) + out_bias[1:2, at]
        ).astype(bf16)
        back_rows(send_c, at)

    arrive(COPY_A, recv_a)
    per_group(forward_group)
    start(COPY_C, send_c, recv_c)
    recv_c[me] = send_c[me]

    def backward_group(g, at):
        along_rows(recv_b, at, inc, g)
        re, im = inc[g, :half], inc[g, half:]
        w_re, w_im = wide[2, g], wide[3, g]
        pre[g, :half] = (
            (dot(re, w_re, (1, 1)) + dot(im, w_im, (1, 1))) * slope[g, :half]
        ).astype(bf16)
        pre[g, half:] = (
            (dot(im, w_re, (1, 1)) - dot(re, w_im, (1, 1))) * slope[g, half:]
        ).astype(bf16)
        re, im = pre[g, :half], pre[g, half:]
        w_re, w_im = wide[0, g], wide[1, g]
        mixed_modes[:half] = (dot(re, w_re, (1, 1)) + dot(im, w_im, (1, 1))).astype(bf16)
        mixed_modes[half:] = (dot(im, w_re, (1, 1)) - dot(re, w_im, (1, 1))).astype(bf16)
        back_rows(send_d, at)

    arrive(COPY_B, recv_b)
    per_group(backward_group)
    start(COPY_D, send_d, recv_d)
    recv_d[me] = send_d[me]

    def fold(product):
        total = jnp.zeros((BLOCK, GROUP), jnp.float32)
        for i in range(PER_GROUP):
            inside = (lane_at >= i * BLOCK) & (lane_at < (i + 1) * BLOCK)
            total = jnp.where(inside, product[i * BLOCK : (i + 1) * BLOCK], total)
        return total.astype(bf16)

    bias_at = lax.broadcasted_iota(jnp.int32, (16, GROUP), 0)

    def grads_group(g, at):
        bias = jnp.zeros((16, GROUP), jnp.float32)
        for k, (left, right) in enumerate(((spec, pre), (hid, inc))):
            a_re, a_im = left[g, :half], left[g, half:]
            b_re, b_im = right[g, :half], right[g, half:]
            first = 2 * k * BLOCK
            grads[first : first + BLOCK, at] = fold(
                dot(a_re, b_re, (0, 0)) + dot(a_im, b_im, (0, 0))
            )
            grads[first + BLOCK : first + 2 * BLOCK, at] = fold(
                dot(a_re, b_im, (0, 0)) - dot(a_im, b_re, (0, 0))
            )
            for c, value in enumerate((b_re, b_im)):
                total = jnp.sum(value.astype(jnp.float32), axis=0, keepdims=True)
                bias = jnp.where(bias_at == 2 * k + c, total, bias)
        grads[4 * BLOCK : 4 * BLOCK + 16, at] = bias.astype(bf16)

    per_group(grads_group)
    halves[...] = dot(picks[...], grads[...]).astype(bf16).reshape(halves.shape)

    def swap(slot, source, target):
        return pltpu.make_async_remote_copy(
            src_ref=source,
            dst_ref=target,
            send_sem=pair_send.at[slot],
            recv_sem=pair_recv.at[slot],
            device_id={"rep": partner},
            device_id_type=MESH_ID,
        )

    first_swap = swap(0, halves.at[partner], half_in)
    first_swap.start()

    def inverse(tokens, table, recv, out):
        for h in range(rows):
            section = recv[:, h * row_chunk : (h + 1) * row_chunk, :]
            product = dot(table[...], section.reshape(n * row_chunk, channels))
            for s in range(samples):
                out[s, h] = (
                    tokens[s, h].astype(jnp.float32)
                    + product[s * padded : s * padded + width]
                ).astype(bf16)

    first_swap.wait()
    send_e[...] = (
        halves[core].astype(jnp.float32) + half_in[...].astype(jnp.float32)
    ).astype(bf16)
    start(COPY_E, send_e, recv_e)
    recv_e[me] = send_e[me]
    arrive(COPY_C, recv_c)
    inverse(tok, inv_mix, recv_c, mixed)

    arrive(COPY_E, recv_e)
    total = jnp.sum(recv_e[...].astype(jnp.float32), axis=0) * (1.0 / divisor)
    bias_out[...] = total
    part[...] = total.astype(bf16)
    each(lambda j: to_peer(COPY_F, lambda peer: part, gathered, j).start())
    gathered[me] = part[...]
    arrive(COPY_D, recv_d)
    inverse(cot, inv_grad, recv_d, grad)
    arrive(COPY_F, gathered)
    last_swap = swap(1, gathered, other)
    last_swap.start()
    weight_out[core] = gathered[...]
    last_swap.wait()
    weight_out[partner] = other[...]

    for phase, source, target in (
        (COPY_A, send_a, recv_a),
        (COPY_B, send_b, recv_b),
        (COPY_C, send_c, recv_c),
        (COPY_D, send_d, recv_d),
        (COPY_E, send_e, recv_e),
    ):
        drain(phase, source, target)
    each(lambda j: to_peer(COPY_F, lambda peer: part, gathered, j).wait_send())


def fits(n, reps, samples, rows, channels):
    per_row = samples * (MODES // n) * 2
    return (
        reps == 2
        and MODES % n == 0
        and per_row % 16 == 0
        and channels % GROUP == 0
        and channels == BLOCKS * BLOCK
        and (4 * BLOCK) % (2 * n) == 0
        and 4 * BLOCK // (2 * n) + 4 <= 16
        and (samples * MODES // n * rows * n) % 16 == 0
    )


def shards(tokens, cotangent, in_weight, in_bias, out_weight, out_bias):
    samples, rows, width, channels = tokens.shape
    n, reps = lax.axis_size("seq"), lax.axis_size("rep")
    if not fits(n, reps, samples, rows, channels):
        return shards_plain(tokens, cotangent, in_weight, in_bias, out_weight, out_bias)
    length = rows * n
    chunk = rows * samples * (MODES // n) * 2
    whole = n * chunk
    groups = channels // GROUP
    per = 4 * BLOCK // (2 * n)
    tables = [jnp.asarray(t) for t in kernel_tables(width, length, n, samples, rows)]
    bf16, f32 = jnp.bfloat16, jnp.float32
    block = pltpu.VMEM((n, chunk, channels), bf16)
    small = pltpu.VMEM((n, 16, channels), bf16)
    kept = pltpu.VMEM((groups, whole, GROUP), bf16)
    vmem = pl.BlockSpec(memory_space=pltpu.VMEM)
    mixed, grad, weight_grad, bias_grad = pl.pallas_call(
        functools.partial(mixer, n, float(samples * reps)),
        out_shape=(
            jax.ShapeDtypeStruct(tokens.shape, bf16),
            jax.ShapeDtypeStruct(tokens.shape, bf16),
            jax.ShapeDtypeStruct((2, n, 16, channels), bf16),
            jax.ShapeDtypeStruct((16, channels), f32),
        ),
        in_specs=[vmem] * 13,
        out_specs=(vmem,) * 4,
        scratch_shapes=[block] * 4
        + [small]
        + [block] * 4
        + [small]
        + [
            pltpu.VMEM((4, groups, GROUP, GROUP), bf16),
            kept,
            kept,
            pltpu.VMEM((groups, whole, GROUP), f32),
            kept,
            kept,
            pltpu.VMEM((whole, GROUP), bf16),
            pltpu.VMEM((4 * BLOCK + 16, channels), bf16),
            pltpu.VMEM((2, n, 16, channels), bf16),
            small,
            pltpu.VMEM((16, channels), bf16),
            small,
            small,
            pltpu.SemaphoreType.DMA((6, n)),
            pltpu.SemaphoreType.DMA((6, n)),
            pltpu.SemaphoreType.DMA((2,)),
            pltpu.SemaphoreType.DMA((2,)),
        ],
        compiler_params=pltpu.CompilerParams(
            collective_id=0, has_side_effects=True, vmem_limit_bytes=63 << 20
        ),
        name="mixer",
    )(tokens, cotangent, *tables, in_weight, in_bias, out_weight, out_bias)
    weights = weight_grad[:, :, :per].reshape(2, 2, BLOCK, BLOCKS, BLOCK)
    weights = weights.transpose(0, 1, 3, 2, 4).astype(f32)
    return (
        mixed,
        grad,
        weights[0],
        bias_grad[per : per + 2],
        weights[1],
        bias_grad[per + 2 : per + 4],
    )


def solution(mesh):
    in_specs = (P("rep", "seq", None, None), P("rep", "seq", None, None), P(), P(), P(), P())
    out_specs = (P("rep", "seq", None, None), P("rep", "seq", None, None), P(), P(), P(), P())
    return jax.shard_map(shards, mesh=mesh, in_specs=in_specs, out_specs=out_specs, check_vma=False)
```

```python
import functools
import math

import jax
import jax.numpy as jnp
import ml_dtypes
import numpy as np
from jax import lax
from jax.experimental import pallas as pl
from jax.experimental.pallas import tpu as pltpu
from jax.sharding import PartitionSpec as P

BLOCKS = 8
BLOCK = 96
MODES = 64


def grid_tables(length, modes):
    position = jnp.arange(length, dtype=jnp.int32)
    frequency = jnp.arange(modes, dtype=jnp.int32)
    residue = position[:, None] * frequency[None, :] % length
    angles = residue.astype(jnp.float32) * (2.0 * math.pi / length)
    factor = 1.0 / math.sqrt(length)
    cosine_table = (jnp.cos(angles) * factor).astype(jnp.bfloat16)
    sine_table = (jnp.sin(angles) * factor).astype(jnp.bfloat16)
    return (cosine_table, sine_table)


def column_tables(grid_width, modes):
    cosine_table, sine_table = grid_tables(grid_width, modes)
    forward = jnp.stack([cosine_table, -sine_table], axis=2)
    doubling = jnp.where(jnp.arange(modes) == 0, 1.0, 2.0).astype(jnp.bfloat16)[:, None]
    inverse = jnp.stack([cosine_table.T * doubling, -(sine_table.T * doubling)], axis=1)
    return (forward, inverse)


def row_table(length):
    cosine_table, sine_table = grid_tables(length, length)
    upper_rows = jnp.stack([cosine_table, sine_table], axis=2)
    lower_rows = jnp.stack([-sine_table, cosine_table], axis=2)
    return jnp.stack([upper_rows, lower_rows], axis=1)


def block_weights(weight):
    real_part, imag_part = (weight[0], weight[1])
    upper_half = jnp.stack([real_part, imag_part], axis=2)
    lower_half = jnp.stack([-imag_part, real_part], axis=2)
    return jnp.stack([upper_half, lower_half], axis=1)


def fold_blocks(blockwise):
    real_part = blockwise[:, 0, :, 0, :] + blockwise[:, 1, :, 1, :]
    imag_part = blockwise[:, 0, :, 1, :] - blockwise[:, 1, :, 0, :]
    return jnp.stack([real_part, imag_part])


def mix_forward(spectrum, weights_in, weights_out, bias_in, bias_out):
    mode_count = spectrum.shape[0] * spectrum.shape[1] * spectrum.shape[2]
    flat_modes = spectrum.reshape(mode_count, 2, BLOCKS, BLOCK)
    hidden_pre = (
        jnp.einsum("mcbi,bciej->mebj", flat_modes, weights_in, preferred_element_type=jnp.float32)
        + bias_in
    )
    hidden = jax.nn.gelu(hidden_pre).astype(jnp.bfloat16)
    spectrum_out = (
        jnp.einsum("mcbi,bciej->mebj", hidden, weights_out, preferred_element_type=jnp.float32)
        + bias_out
    )
    return (
        flat_modes,
        hidden_pre,
        hidden,
        spectrum_out.astype(jnp.bfloat16).reshape(spectrum.shape),
    )


def mix_backward(flat_modes, hidden_pre, hidden, incoming, weights_in, weights_out):
    incoming_flat = incoming.reshape(flat_modes.shape)
    out_bias_part = jnp.sum(incoming_flat.astype(jnp.float32), axis=0).reshape(2, -1)
    out_weight_part = fold_blocks(
        jnp.einsum("mcbi,mebj->bciej", hidden, incoming_flat, preferred_element_type=jnp.float32)
    )
    hidden_grad = jnp.einsum(
        "mebj,bciej->mcbi", incoming_flat, weights_out, preferred_element_type=jnp.float32
    )
    pre_grad = jax.vjp(jax.nn.gelu, hidden_pre)[1](hidden_grad)[0].astype(jnp.bfloat16)
    in_bias_part = jnp.sum(pre_grad.astype(jnp.float32), axis=0).reshape(2, -1)
    in_weight_part = fold_blocks(
        jnp.einsum("mcbi,mebj->bciej", flat_modes, pre_grad, preferred_element_type=jnp.float32)
    )
    spectrum_grad = jnp.einsum(
        "mebj,bciej->mcbi", pre_grad, weights_in, preferred_element_type=jnp.float32
    )
    spectrum_grad = spectrum_grad.astype(jnp.bfloat16).reshape(incoming.shape)
    return (spectrum_grad, (in_weight_part, in_bias_part, out_weight_part, out_bias_part))


def shards_plain(tokens, cotangent, in_weight, in_bias, out_weight, out_bias):
    samples, row_count, grid_width, channels = tokens.shape
    length = row_count * lax.axis_size("seq")
    column_forward, column_inverse = column_tables(grid_width, MODES)
    row_matrix = row_table(length)
    weights_in = block_weights(in_weight)
    weights_out = block_weights(out_weight)
    bias_in = in_bias.reshape(2, BLOCKS, BLOCK)
    bias_out = out_bias.reshape(2, BLOCKS, BLOCK)

    def along_rows(section):
        return jnp.einsum(
            "qehc,shkcd->sqked", row_matrix, section, preferred_element_type=jnp.float32
        ).astype(jnp.bfloat16)

    def back_rows(section):
        return jnp.einsum(
            "qehc,sqked->shkcd", row_matrix, section, preferred_element_type=jnp.float32
        ).astype(jnp.bfloat16)

    spec_rows = jnp.einsum(
        "shwd,wkc->shkcd", tokens, column_forward, preferred_element_type=jnp.float32
    ).astype(jnp.bfloat16)
    spectrum = along_rows(lax.all_to_all(spec_rows, "seq", split_axis=2, concat_axis=1, tiled=True))
    flat_modes, hidden_pre, hidden, spectrum_out = mix_forward(
        spectrum, weights_in, weights_out, bias_in, bias_out
    )
    mixed_grid = jnp.einsum(
        "shkcd,kcw->shwd",
        lax.all_to_all(back_rows(spectrum_out), "seq", split_axis=1, concat_axis=2, tiled=True),
        column_inverse,
        preferred_element_type=jnp.float32,
    )
    cot_rows = jnp.einsum(
        "shwd,kcw->shkcd", cotangent, column_inverse, preferred_element_type=jnp.float32
    ).astype(jnp.bfloat16)
    incoming = along_rows(lax.all_to_all(cot_rows, "seq", split_axis=2, concat_axis=1, tiled=True))
    spectrum_grad, partials = mix_backward(
        flat_modes, hidden_pre, hidden, incoming, weights_in, weights_out
    )
    adjoint_part = jnp.einsum(
        "shkcd,wkc->shwd",
        lax.all_to_all(back_rows(spectrum_grad), "seq", split_axis=1, concat_axis=2, tiled=True),
        column_forward,
        preferred_element_type=jnp.float32,
    )
    mixed_out = (tokens.astype(jnp.float32) + mixed_grid).astype(jnp.bfloat16)
    tokens_grad = (cotangent.astype(jnp.float32) + adjoint_part).astype(jnp.bfloat16)
    totals = lax.psum((partials[0], partials[1], partials[2], partials[3]), ("seq", "rep"))
    divisor = float(samples * lax.axis_size("rep"))
    return (
        mixed_out,
        tokens_grad,
        totals[0] / divisor,
        totals[1] / divisor,
        totals[2] / divisor,
        totals[3] / divisor,
    )


GROUP = math.lcm(BLOCK, 128)
PER_GROUP = GROUP // BLOCK
COPY_A, COPY_B, COPY_C, COPY_E, COPY_F, COPY_G, COPY_H, COPY_D = range(8)
MESH_ID = pl.DeviceIdType.MESH


def host_tables(length, modes):
    residue = np.arange(length)[:, None] * np.arange(modes)[None, :] % length
    angles = residue.astype(np.float32) * np.float32(2.0 * math.pi / length)
    factor = np.float32(1.0 / math.sqrt(length))
    rounded = [(f(angles) * factor).astype(ml_dtypes.bfloat16) for f in (np.cos, np.sin)]
    return [table.astype(np.float32) for table in rounded]


def kernel_tables(width, length, n, samples, rows):
    local = MODES // n
    cosine, sine = host_tables(width, MODES)
    forward = np.stack([cosine.T, -sine.T], axis=1)
    doubled = forward * np.where(np.arange(MODES) == 0, 1.0, 2.0)[:, None, None]

    def spread(table):
        table = table.reshape(n, local, 2, width)
        whole = np.zeros((n, samples, local, 2, width, samples), np.float32)
        for s in range(samples):
            whole[:, s, :, :, :, s] = table
        return whole.reshape(n * samples * local * 2, width * samples)

    cosine, sine = host_tables(length, length)
    upper = np.stack([cosine, sine], axis=2)
    lower = np.stack([-sine, cosine], axis=2)
    turn = np.stack([upper, lower], axis=0)
    both = samples * local
    mixing = np.zeros((2, both, length, length, both, 2), np.float32)
    for x in range(both):
        mixing[:, x, :, :, x, :] = turn
    mixing = mixing.reshape(2 * both * length, length * both * 2)

    flat = [
        spread(forward),
        spread(doubled),
        spread(doubled).T,
        spread(forward).T,
        mixing,
    ]
    return [np.ascontiguousarray(t).astype(ml_dtypes.bfloat16) for t in flat]


def dot(a, b, contract=(1, 0)):
    return lax.dot_general(
        a, b, (((contract[0],), (contract[1],)), ((), ())), preferred_element_type=jnp.float32
    )


def mixer(
    n,
    inner,
    divisor,
    tok,
    cot,
    col_tok,
    col_cot,
    inv_mix,
    inv_grad,
    turn,
    in_weight,
    in_bias,
    out_weight,
    out_bias,
    mixed,
    grad,
    weight_out,
    bias_out,
    send_a,
    send_b,
    send_c,
    send_d,
    send_e,
    send_f,
    recv_a,
    recv_b,
    recv_c,
    recv_d,
    recv_e,
    recv_f,
    turn_back,
    wide,
    spec,
    hid,
    slope,
    inc,
    pre,
    mixed_modes,
    grads,
    halves,
    half_in,
    part,
    gathered,
    other,
    send_sem,
    recv_sem,
    pair_send,
    pair_recv,
):
    me = lax.axis_index("seq")
    core = lax.axis_index("rep")
    partner = 1 - core
    rows, width, samples, channels = tok.shape
    groups = channels // GROUP
    outer = n // inner
    across, within = me // inner, lax.rem(me, inner)
    chunk = send_a.shape[1]
    row_chunk = chunk // rows
    bf16 = jnp.bfloat16

    barrier = pltpu.get_barrier_semaphore()

    def greet(j, carry):
        peer = lax.rem(me + j, n)
        pl.semaphore_signal(barrier, inc=1, device_id={"seq": peer}, device_id_type=MESH_ID)
        return carry

    lax.fori_loop(1, n, greet, 0)
    pl.semaphore_signal(barrier, inc=1, device_id={"rep": partner}, device_id_type=MESH_ID)

    def copy_to(phase, peer, mine, source, target):
        return pltpu.make_async_remote_copy(
            src_ref=source,
            dst_ref=target,
            send_sem=send_sem.at[phase, peer],
            recv_sem=recv_sem.at[phase, mine],
            device_id={"seq": peer},
            device_id_type=MESH_ID,
        )

    def loop(count, act):
        def step(j, carry):
            act(j)
            return carry

        lax.fori_loop(1, count, step, 0)

    def peer_at(j):
        return lax.rem(me + j, n)

    def plane_at(j):
        return lax.rem(within + j, inner)

    def line_at(j):
        return lax.rem(across + j, outer)

    def everyone(phase, source, target, at=None):
        cut = (lambda ref, i: ref.at[i]) if at is None else (lambda ref, i: ref.at[i, at])

        def out(j):
            peer = peer_at(j)
            return copy_to(phase, peer, me, cut(source, peer), cut(target, me))

        def back(j):
            peer = peer_at(j)
            return copy_to(phase, peer, peer, cut(source, peer), cut(target, peer))

        return (
            lambda: loop(n, lambda j: out(j).start()),
            lambda: loop(n, lambda j: back(j).wait_recv()),
            lambda: loop(n, lambda j: out(j).wait_send()),
        )

    def plane(phase, source, target):
        def out(j):
            v = plane_at(j)
            peer = across * inner + v
            return copy_to(phase, peer, me, source(v), target(within))

        def back(j):
            v = plane_at(j)
            peer = across * inner + v
            return copy_to(phase, peer, peer, source(v), target(v))

        return (
            lambda: loop(inner, lambda j: out(j).start()),
            lambda: loop(inner, lambda j: back(j).wait_recv()),
            lambda: loop(inner, lambda j: out(j).wait_send()),
        )

    def line(phase, source, target):
        def out(j):
            z = line_at(j)
            peer = z * inner + within
            return copy_to(phase, peer, me, source(z), target(across))

        def back(j):
            z = line_at(j)
            peer = z * inner + within
            return copy_to(phase, peer, peer, source(z), target(z))

        return (
            lambda: loop(outer, lambda j: out(j).start()),
            lambda: loop(outer, lambda j: back(j).wait_recv()),
            lambda: loop(outer, lambda j: out(j).wait_send()),
        )

    move_a = everyone(COPY_A, send_a, recv_a)
    move_b = everyone(COPY_B, send_b, recv_b)
    move_c = everyone(COPY_C, send_c, recv_c)
    pieces = [
        everyone(COPY_D + h, send_d, recv_d, pl.ds(h * row_chunk, row_chunk))
        for h in range(rows)
    ]
    move_e = plane(COPY_E, lambda v: send_e.at[v], lambda v: recv_e.at[v])
    move_f = line(COPY_F, lambda z: send_f.at[z], lambda z: recv_f.at[z])
    move_g = line(COPY_G, lambda z: part, lambda z: gathered.at[within, z])
    move_h = plane(COPY_H, lambda v: gathered.at[within], lambda v: gathered.at[v])

    def columns(tokens, table, send):
        for h in range(rows):
            product = dot(table[...], tokens[h].reshape(width * samples, channels))
            send[:, h * row_chunk : (h + 1) * row_chunk, :] = product.astype(bf16).reshape(
                n, row_chunk, channels
            )

    columns(tok, col_tok, send_a)
    pl.semaphore_wait(barrier, n)
    move_a[0]()
    columns(cot, col_cot, send_b)
    move_b[0]()
    recv_a[me] = send_a[me]
    recv_b[me] = send_b[me]

    turn_back[...] = turn[...].T
    row_at = lax.broadcasted_iota(jnp.int32, (BLOCK, GROUP), 0)
    lane_at = lax.broadcasted_iota(jnp.int32, (BLOCK, GROUP), 1)
    for at, weight in enumerate((in_weight, out_weight)):
        for i in range(PER_GROUP):
            place = (lane_at == row_at + i * BLOCK).astype(bf16)
            for c in range(2):
                for g in range(groups):
                    wide[2 * at + c, g, i * BLOCK : (i + 1) * BLOCK, :] = dot(
                        weight[c, g * PER_GROUP + i], place
                    ).astype(bf16)

    half = turn.shape[0] // 2
    scale = math.sqrt(2.0 / math.pi)

    def lanes(g):
        return pl.ds(pl.multiple_of(g * GROUP, GROUP), GROUP)

    def per_group(act):
        def step(g, carry):
            act(g, lanes(g))
            return carry

        lax.fori_loop(0, groups, step, 0)

    def along_rows(recv, at, keep, g):
        keep[g] = dot(turn[...], recv[:, :, at].reshape(turn.shape[1], GROUP)).astype(bf16)

    def back_rows(send, at):
        send[:, :, at] = (
            dot(turn_back[...], mixed_modes[...]).astype(bf16).reshape(n, chunk, GROUP)
        )

    def forward_group(g, at):
        along_rows(recv_a, at, spec, g)
        re, im = spec[g, :half], spec[g, half:]
        w_re, w_im = wide[0, g], wide[1, g]
        for c in range(2):
            if c == 0:
                value = dot(re, w_re) - dot(im, w_im)
            else:
                value = dot(re, w_im) + dot(im, w_re)
            value = value + in_bias[c : c + 1, at]
            square = value * value
            tanh = jnp.tanh(scale * value * (1.0 + 0.044715 * square))
            hid[g, c * half : (c + 1) * half] = (0.5 * value * (1.0 + tanh)).astype(bf16)
            slope[g, c * half : (c + 1) * half] = 0.5 * (1.0 + tanh) + 0.5 * value * (
                1.0 - tanh * tanh
            ) * (scale * (1.0 + (3.0 * 0.044715) * square))
        re, im = hid[g, :half], hid[g, half:]
        w_re, w_im = wide[2, g], wide[3, g]
        mixed_modes[:half] = (
            dot(re, w_re) - dot(im, w_im) + out_bias[0:1, at]
        ).astype(bf16)
        mixed_modes[half:] = (
            dot(re, w_im) + dot(im, w_re) + out_bias[1:2, at]
        ).astype(bf16)
        back_rows(send_c, at)

    move_a[1]()
    per_group(forward_group)
    move_c[0]()
    recv_c[me] = send_c[me]

    def backward_group(g, at):
        along_rows(recv_b, at, inc, g)
        re, im = inc[g, :half], inc[g, half:]
        w_re, w_im = wide[2, g], wide[3, g]
        pre[g, :half] = (
            (dot(re, w_re, (1, 1)) + dot(im, w_im, (1, 1))) * slope[g, :half]
        ).astype(bf16)
        pre[g, half:] = (
            (dot(im, w_re, (1, 1)) - dot(re, w_im, (1, 1))) * slope[g, half:]
        ).astype(bf16)
        re, im = pre[g, :half], pre[g, half:]
        w_re, w_im = wide[0, g], wide[1, g]
        mixed_modes[:half] = (dot(re, w_re, (1, 1)) + dot(im, w_im, (1, 1))).astype(bf16)
        mixed_modes[half:] = (dot(im, w_re, (1, 1)) - dot(re, w_im, (1, 1))).astype(bf16)
        back_rows(send_d, at)

    move_b[1]()
    per_group(backward_group)

    def fold(product):
        total = jnp.zeros((BLOCK, GROUP), jnp.float32)
        for i in range(PER_GROUP):
            inside = (lane_at >= i * BLOCK) & (lane_at < (i + 1) * BLOCK)
            total = jnp.where(inside, product[i * BLOCK : (i + 1) * BLOCK], total)
        return total.astype(bf16)

    bias_at = lax.broadcasted_iota(jnp.int32, (16, GROUP), 0)

    def grads_group(g, at):
        bias = jnp.zeros((16, GROUP), jnp.float32)
        for k, (left, right) in enumerate(((spec, pre), (hid, inc))):
            a_re, a_im = left[g, :half], left[g, half:]
            b_re, b_im = right[g, :half], right[g, half:]
            first = 2 * k * BLOCK
            grads[first : first + BLOCK, at] = fold(
                dot(a_re, b_re, (0, 0)) + dot(a_im, b_im, (0, 0))
            )
            grads[first + BLOCK : first + 2 * BLOCK, at] = fold(
                dot(a_re, b_im, (0, 0)) - dot(a_im, b_re, (0, 0))
            )
            for c, value in enumerate((b_re, b_im)):
                total = jnp.sum(value.astype(jnp.float32), axis=0, keepdims=True)
                bias = jnp.where(bias_at == 2 * k + c, total, bias)
        grads[4 * BLOCK : 4 * BLOCK + 16, at] = bias.astype(bf16)

    per_group(grads_group)
    per = 4 * BLOCK // (2 * n)
    to_row = lax.broadcasted_iota(jnp.int32, (2 * n * 16, 4 * BLOCK + 16), 0)
    from_row = lax.broadcasted_iota(jnp.int32, (2 * n * 16, 4 * BLOCK + 16), 1)
    slot = to_row % 16
    wanted = jnp.where(slot < per, to_row // 16 * per + slot, 4 * BLOCK + slot - per)
    picks = (wanted == from_row).astype(bf16)
    halves[...] = dot(picks, grads[...]).astype(bf16).reshape(halves.shape)

    def swap(slot, source, target):
        return pltpu.make_async_remote_copy(
            src_ref=source,
            dst_ref=target,
            send_sem=pair_send.at[slot],
            recv_sem=pair_recv.at[slot],
            device_id={"rep": partner},
            device_id_type=MESH_ID,
        )

    first_swap = swap(0, halves.at[partner], half_in)
    first_swap.start()

    def inverse_row(h, tokens, table, recv, out):
        section = recv[:, h * row_chunk : (h + 1) * row_chunk, :]
        product = dot(table[...], section.reshape(n * row_chunk, channels))
        kept = tokens[h].reshape(width * samples, channels).astype(jnp.float32)
        out[h] = (kept + product).astype(bf16).reshape(width, samples, channels)

    def inverse(tokens, table, recv, out):
        for h in range(rows):
            inverse_row(h, tokens, table, recv, out)

    first_swap.wait()
    send_e[...] = (
        (halves[core].astype(jnp.float32) + half_in[...].astype(jnp.float32))
        .astype(bf16)
        .reshape(send_e.shape)
    )
    move_e[0]()
    recv_e[within] = send_e[within]
    pieces[0][0]()
    recv_d[me] = send_d[me]
    move_c[1]()
    inverse(tok, inv_mix, recv_c, mixed)

    move_e[1]()
    send_f[...] = jnp.sum(recv_e[...].astype(jnp.float32), axis=0).astype(bf16)
    move_f[0]()
    recv_f[across] = send_f[across]
    middle = max(2, rows - 1)
    for piece in pieces[1:middle]:
        piece[0]()
    move_f[1]()
    total = jnp.sum(recv_f[...].astype(jnp.float32), axis=0) * (1.0 / divisor)
    bias_out[...] = total
    part[...] = total.astype(bf16)
    move_g[0]()
    gathered[within, across] = part[...]
    for piece in pieces[middle:]:
        piece[0]()
    pieces[0][1]()
    inverse_row(0, cot, inv_grad, recv_d, grad)
    move_g[1]()
    move_h[0]()
    for h in range(1, rows - 1):
        pieces[h][1]()
        inverse_row(h, cot, inv_grad, recv_d, grad)
    move_h[1]()
    last_swap = swap(1, gathered, other)
    last_swap.start()
    flat = (n, 16, channels)
    weight_out[core] = gathered[...].reshape(flat)
    for h in range(max(1, rows - 1), rows):
        pieces[h][1]()
        inverse_row(h, cot, inv_grad, recv_d, grad)
    last_swap.wait()
    weight_out[partner] = other[...].reshape(flat)

    for move in (move_a, move_b, move_c, move_e, move_f, move_g, move_h, *pieces):
        move[2]()


def fits(n, reps, samples, rows, channels):
    per_row = samples * (MODES // n) * 2
    return (
        reps == 2
        and MODES % n == 0
        and per_row % 16 == 0
        and channels % GROUP == 0
        and channels == BLOCKS * BLOCK
        and (4 * BLOCK) % (2 * n) == 0
        and n > 1
        and n & (n - 1) == 0
        and rows > 1
        and 4 * BLOCK // (2 * n) + 4 <= 16
        and (samples * MODES // n * rows * n) % 16 == 0
    )


def shards(tokens, cotangent, in_weight, in_bias, out_weight, out_bias):
    samples, rows, width, channels = tokens.shape
    n, reps = lax.axis_size("seq"), lax.axis_size("rep")
    if not fits(n, reps, samples, rows, channels):
        return shards_plain(tokens, cotangent, in_weight, in_bias, out_weight, out_bias)
    length = rows * n
    inner = 2 ** ((n.bit_length() - 1) // 2)
    outer = n // inner
    chunk = rows * samples * (MODES // n) * 2
    whole = n * chunk
    groups = channels // GROUP
    per = 4 * BLOCK // (2 * n)
    tables = [jnp.asarray(t) for t in kernel_tables(width, length, n, samples, rows)]
    bf16, f32 = jnp.bfloat16, jnp.float32
    block = pltpu.VMEM((n, chunk, channels), bf16)
    small = pltpu.VMEM((n, 16, channels), bf16)
    ringed = pltpu.VMEM((inner, outer, 16, channels), bf16)
    lined = pltpu.VMEM((outer, 16, channels), bf16)
    planes = (tokens.transpose(1, 2, 0, 3), cotangent.transpose(1, 2, 0, 3))
    kept = pltpu.VMEM((groups, whole, GROUP), bf16)
    vmem = pl.BlockSpec(memory_space=pltpu.VMEM)
    mixed, grad, weight_grad, bias_grad = pl.pallas_call(
        functools.partial(mixer, n, inner, float(samples * reps)),
        out_shape=(
            jax.ShapeDtypeStruct(planes[0].shape, bf16),
            jax.ShapeDtypeStruct(planes[1].shape, bf16),
            jax.ShapeDtypeStruct((2, n, 16, channels), bf16),
            jax.ShapeDtypeStruct((16, channels), f32),
        ),
        in_specs=[vmem] * 11,
        out_specs=(vmem,) * 4,
        scratch_shapes=[block] * 4
        + [ringed, lined]
        + [block] * 4
        + [ringed, lined]
        + [
            pltpu.VMEM((whole, whole), bf16),
            pltpu.VMEM((4, groups, GROUP, GROUP), bf16),
            kept,
            kept,
            pltpu.VMEM((groups, whole, GROUP), f32),
            kept,
            kept,
            pltpu.VMEM((whole, GROUP), bf16),
            pltpu.VMEM((4 * BLOCK + 16, channels), bf16),
            pltpu.VMEM((2, n, 16, channels), bf16),
            small,
            pltpu.VMEM((16, channels), bf16),
            ringed,
            ringed,
            pltpu.SemaphoreType.DMA((COPY_D + rows, n)),
            pltpu.SemaphoreType.DMA((COPY_D + rows, n)),
            pltpu.SemaphoreType.DMA((2,)),
            pltpu.SemaphoreType.DMA((2,)),
        ],
        compiler_params=pltpu.CompilerParams(
            collective_id=0, has_side_effects=True, vmem_limit_bytes=63 << 20
        ),
        name="mixer",
    )(*planes, *tables, in_weight, in_bias, out_weight, out_bias)
    weights = weight_grad[:, :, :per].reshape(2, 2, BLOCK, BLOCKS, BLOCK)
    weights = weights.transpose(0, 1, 3, 2, 4).astype(f32)
    return (
        mixed.transpose(2, 0, 1, 3),
        grad.transpose(2, 0, 1, 3),
        weights[0],
        bias_grad[per : per + 2],
        weights[1],
        bias_grad[per + 2 : per + 4],
    )


def solution(mesh):
    in_specs = (P("rep", "seq", None, None), P("rep", "seq", None, None), P(), P(), P(), P())
    out_specs = (P("rep", "seq", None, None), P("rep", "seq", None, None), P(), P(), P(), P())
    return jax.shard_map(shards, mesh=mesh, in_specs=in_specs, out_specs=out_specs, check_vma=False)
```

```python
import functools
import math

import jax
import jax.numpy as jnp
import ml_dtypes
import numpy as np
from jax import lax
from jax.experimental import pallas as pl
from jax.experimental.pallas import tpu as pltpu
from jax.sharding import PartitionSpec as P

BLOCKS = 8
BLOCK = 96
MODES = 64


def grid_tables(length, modes):
    position = jnp.arange(length, dtype=jnp.int32)
    frequency = jnp.arange(modes, dtype=jnp.int32)
    residue = position[:, None] * frequency[None, :] % length
    angles = residue.astype(jnp.float32) * (2.0 * math.pi / length)
    factor = 1.0 / math.sqrt(length)
    cosine_table = (jnp.cos(angles) * factor).astype(jnp.bfloat16)
    sine_table = (jnp.sin(angles) * factor).astype(jnp.bfloat16)
    return (cosine_table, sine_table)


def column_tables(grid_width, modes):
    cosine_table, sine_table = grid_tables(grid_width, modes)
    forward = jnp.stack([cosine_table, -sine_table], axis=2)
    doubling = jnp.where(jnp.arange(modes) == 0, 1.0, 2.0).astype(jnp.bfloat16)[:, None]
    inverse = jnp.stack([cosine_table.T * doubling, -(sine_table.T * doubling)], axis=1)
    return (forward, inverse)


def row_table(length):
    cosine_table, sine_table = grid_tables(length, length)
    upper_rows = jnp.stack([cosine_table, sine_table], axis=2)
    lower_rows = jnp.stack([-sine_table, cosine_table], axis=2)
    return jnp.stack([upper_rows, lower_rows], axis=1)


def block_weights(weight):
    real_part, imag_part = (weight[0], weight[1])
    upper_half = jnp.stack([real_part, imag_part], axis=2)
    lower_half = jnp.stack([-imag_part, real_part], axis=2)
    return jnp.stack([upper_half, lower_half], axis=1)


def fold_blocks(blockwise):
    real_part = blockwise[:, 0, :, 0, :] + blockwise[:, 1, :, 1, :]
    imag_part = blockwise[:, 0, :, 1, :] - blockwise[:, 1, :, 0, :]
    return jnp.stack([real_part, imag_part])


def mix_forward(spectrum, weights_in, weights_out, bias_in, bias_out):
    mode_count = spectrum.shape[0] * spectrum.shape[1] * spectrum.shape[2]
    flat_modes = spectrum.reshape(mode_count, 2, BLOCKS, BLOCK)
    hidden_pre = (
        jnp.einsum("mcbi,bciej->mebj", flat_modes, weights_in, preferred_element_type=jnp.float32)
        + bias_in
    )
    hidden = jax.nn.gelu(hidden_pre).astype(jnp.bfloat16)
    spectrum_out = (
        jnp.einsum("mcbi,bciej->mebj", hidden, weights_out, preferred_element_type=jnp.float32)
        + bias_out
    )
    return (
        flat_modes,
        hidden_pre,
        hidden,
        spectrum_out.astype(jnp.bfloat16).reshape(spectrum.shape),
    )


def mix_backward(flat_modes, hidden_pre, hidden, incoming, weights_in, weights_out):
    incoming_flat = incoming.reshape(flat_modes.shape)
    out_bias_part = jnp.sum(incoming_flat.astype(jnp.float32), axis=0).reshape(2, -1)
    out_weight_part = fold_blocks(
        jnp.einsum("mcbi,mebj->bciej", hidden, incoming_flat, preferred_element_type=jnp.float32)
    )
    hidden_grad = jnp.einsum(
        "mebj,bciej->mcbi", incoming_flat, weights_out, preferred_element_type=jnp.float32
    )
    pre_grad = jax.vjp(jax.nn.gelu, hidden_pre)[1](hidden_grad)[0].astype(jnp.bfloat16)
    in_bias_part = jnp.sum(pre_grad.astype(jnp.float32), axis=0).reshape(2, -1)
    in_weight_part = fold_blocks(
        jnp.einsum("mcbi,mebj->bciej", flat_modes, pre_grad, preferred_element_type=jnp.float32)
    )
    spectrum_grad = jnp.einsum(
        "mebj,bciej->mcbi", pre_grad, weights_in, preferred_element_type=jnp.float32
    )
    spectrum_grad = spectrum_grad.astype(jnp.bfloat16).reshape(incoming.shape)
    return (spectrum_grad, (in_weight_part, in_bias_part, out_weight_part, out_bias_part))


def shards_plain(tokens, cotangent, in_weight, in_bias, out_weight, out_bias):
    samples, row_count, grid_width, channels = tokens.shape
    length = row_count * lax.axis_size("seq")
    column_forward, column_inverse = column_tables(grid_width, MODES)
    row_matrix = row_table(length)
    weights_in = block_weights(in_weight)
    weights_out = block_weights(out_weight)
    bias_in = in_bias.reshape(2, BLOCKS, BLOCK)
    bias_out = out_bias.reshape(2, BLOCKS, BLOCK)

    def along_rows(section):
        return jnp.einsum(
            "qehc,shkcd->sqked", row_matrix, section, preferred_element_type=jnp.float32
        ).astype(jnp.bfloat16)

    def back_rows(section):
        return jnp.einsum(
            "qehc,sqked->shkcd", row_matrix, section, preferred_element_type=jnp.float32
        ).astype(jnp.bfloat16)

    spec_rows = jnp.einsum(
        "shwd,wkc->shkcd", tokens, column_forward, preferred_element_type=jnp.float32
    ).astype(jnp.bfloat16)
    spectrum = along_rows(lax.all_to_all(spec_rows, "seq", split_axis=2, concat_axis=1, tiled=True))
    flat_modes, hidden_pre, hidden, spectrum_out = mix_forward(
        spectrum, weights_in, weights_out, bias_in, bias_out
    )
    mixed_grid = jnp.einsum(
        "shkcd,kcw->shwd",
        lax.all_to_all(back_rows(spectrum_out), "seq", split_axis=1, concat_axis=2, tiled=True),
        column_inverse,
        preferred_element_type=jnp.float32,
    )
    cot_rows = jnp.einsum(
        "shwd,kcw->shkcd", cotangent, column_inverse, preferred_element_type=jnp.float32
    ).astype(jnp.bfloat16)
    incoming = along_rows(lax.all_to_all(cot_rows, "seq", split_axis=2, concat_axis=1, tiled=True))
    spectrum_grad, partials = mix_backward(
        flat_modes, hidden_pre, hidden, incoming, weights_in, weights_out
    )
    adjoint_part = jnp.einsum(
        "shkcd,wkc->shwd",
        lax.all_to_all(back_rows(spectrum_grad), "seq", split_axis=1, concat_axis=2, tiled=True),
        column_forward,
        preferred_element_type=jnp.float32,
    )
    mixed_out = (tokens.astype(jnp.float32) + mixed_grid).astype(jnp.bfloat16)
    tokens_grad = (cotangent.astype(jnp.float32) + adjoint_part).astype(jnp.bfloat16)
    totals = lax.psum((partials[0], partials[1], partials[2], partials[3]), ("seq", "rep"))
    divisor = float(samples * lax.axis_size("rep"))
    return (
        mixed_out,
        tokens_grad,
        totals[0] / divisor,
        totals[1] / divisor,
        totals[2] / divisor,
        totals[3] / divisor,
    )


GROUP = math.lcm(BLOCK, 128)
PER_GROUP = GROUP // BLOCK
COPY_A, COPY_B, COPY_C, COPY_E, COPY_F, COPY_G, COPY_H, COPY_D = range(8)
MESH_ID = pl.DeviceIdType.MESH


def host_tables(length, modes):
    residue = np.arange(length)[:, None] * np.arange(modes)[None, :] % length
    angles = residue.astype(np.float32) * np.float32(2.0 * math.pi / length)
    factor = np.float32(1.0 / math.sqrt(length))
    rounded = [(f(angles) * factor).astype(ml_dtypes.bfloat16) for f in (np.cos, np.sin)]
    return [table.astype(np.float32) for table in rounded]


def kernel_tables(width, length, n, samples, rows):
    local = MODES // n
    cosine, sine = host_tables(width, MODES)
    forward = np.stack([cosine.T, -sine.T], axis=1)
    doubled = forward * np.where(np.arange(MODES) == 0, 1.0, 2.0)[:, None, None]

    def spread(table):
        table = table.reshape(n, local, 2, width)
        whole = np.zeros((n, samples, local, 2, width, samples), np.float32)
        for s in range(samples):
            whole[:, s, :, :, :, s] = table
        return whole.reshape(n * samples * local * 2, width * samples)

    cosine, sine = host_tables(length, length)
    upper = np.stack([cosine, sine], axis=2)
    lower = np.stack([-sine, cosine], axis=2)
    turn = np.stack([upper, lower], axis=0)
    both = samples * local
    mixing = np.zeros((2, both, length, length, both, 2), np.float32)
    for x in range(both):
        mixing[:, x, :, :, x, :] = turn
    mixing = mixing.reshape(2 * both * length, length * both * 2)

    flat = [
        spread(forward),
        spread(doubled),
        spread(doubled).T,
        spread(forward).T,
        mixing,
    ]
    return [np.ascontiguousarray(t).astype(ml_dtypes.bfloat16) for t in flat]


def dot(a, b, contract=(1, 0)):
    return lax.dot_general(
        a, b, (((contract[0],), (contract[1],)), ((), ())), preferred_element_type=jnp.float32
    )


def mixer(
    n,
    inner,
    divisor,
    tok,
    cot,
    col_tok,
    col_cot,
    inv_mix,
    inv_grad,
    turn,
    in_weight,
    in_bias,
    out_weight,
    out_bias,
    mixed,
    grad,
    in_weight_grad,
    in_bias_grad,
    out_weight_grad,
    out_bias_grad,
    send_a,
    send_b,
    send_c,
    send_d,
    send_e,
    send_f,
    recv_a,
    recv_b,
    recv_c,
    recv_d,
    recv_e,
    recv_f,
    turn_back,
    wide,
    spec,
    hid,
    slope,
    inc,
    pre,
    mixed_modes,
    grads,
    halves,
    half_in,
    part,
    gathered,
    other,
    both,
    send_sem,
    recv_sem,
    pair_send,
    pair_recv,
):
    me = lax.axis_index("seq")
    core = lax.axis_index("rep")
    partner = 1 - core
    rows, width, samples, channels = tok.shape
    groups = channels // GROUP
    outer = n // inner
    across, within = me // inner, lax.rem(me, inner)
    chunk = send_a.shape[1]
    row_chunk = chunk // rows
    bf16 = jnp.bfloat16

    barrier = pltpu.get_barrier_semaphore()

    def greet(j, carry):
        peer = lax.rem(me + j, n)
        pl.semaphore_signal(barrier, inc=1, device_id={"seq": peer}, device_id_type=MESH_ID)
        return carry

    lax.fori_loop(1, n, greet, 0)
    pl.semaphore_signal(barrier, inc=1, device_id={"rep": partner}, device_id_type=MESH_ID)

    def copy_to(phase, peer, mine, source, target):
        return pltpu.make_async_remote_copy(
            src_ref=source,
            dst_ref=target,
            send_sem=send_sem.at[phase, peer],
            recv_sem=recv_sem.at[phase, mine],
            device_id={"seq": peer},
            device_id_type=MESH_ID,
        )

    def loop(count, act):
        def step(j, carry):
            act(j)
            return carry

        lax.fori_loop(1, count, step, 0)

    def peer_at(j):
        return lax.rem(me + j, n)

    def plane_at(j):
        return lax.rem(within + j, inner)

    def line_at(j):
        return lax.rem(across + j, outer)

    def everyone(phase, source, target, at=None):
        cut = (lambda ref, i: ref.at[i]) if at is None else (lambda ref, i: ref.at[i, at])

        def out(j):
            peer = peer_at(j)
            return copy_to(phase, peer, me, cut(source, peer), cut(target, me))

        def back(j):
            peer = peer_at(j)
            return copy_to(phase, peer, peer, cut(source, peer), cut(target, peer))

        return (
            lambda: loop(n, lambda j: out(j).start()),
            lambda: loop(n, lambda j: back(j).wait_recv()),
            lambda: loop(n, lambda j: out(j).wait_send()),
        )

    def plane(phase, source, target):
        def out(j):
            v = plane_at(j)
            peer = across * inner + v
            return copy_to(phase, peer, me, source(v), target(within))

        def back(j):
            v = plane_at(j)
            peer = across * inner + v
            return copy_to(phase, peer, peer, source(v), target(v))

        return (
            lambda: loop(inner, lambda j: out(j).start()),
            lambda: loop(inner, lambda j: back(j).wait_recv()),
            lambda: loop(inner, lambda j: out(j).wait_send()),
        )

    def line(phase, source, target):
        def out(j):
            z = line_at(j)
            peer = z * inner + within
            return copy_to(phase, peer, me, source(z), target(across))

        def back(j):
            z = line_at(j)
            peer = z * inner + within
            return copy_to(phase, peer, peer, source(z), target(z))

        return (
            lambda: loop(outer, lambda j: out(j).start()),
            lambda: loop(outer, lambda j: back(j).wait_recv()),
            lambda: loop(outer, lambda j: out(j).wait_send()),
        )

    move_a = everyone(COPY_A, send_a, recv_a)
    move_b = everyone(COPY_B, send_b, recv_b)
    move_c = everyone(COPY_C, send_c, recv_c)
    pieces = [
        everyone(COPY_D + h, send_d, recv_d, pl.ds(h * row_chunk, row_chunk))
        for h in range(rows)
    ]
    move_e = plane(COPY_E, lambda v: send_e.at[v], lambda v: recv_e.at[v])
    move_f = line(COPY_F, lambda z: send_f.at[z], lambda z: recv_f.at[z])
    move_g = line(COPY_G, lambda z: part, lambda z: gathered.at[within, z])
    move_h = plane(COPY_H, lambda v: gathered.at[within], lambda v: gathered.at[v])

    def columns(tokens, table, send):
        for h in range(rows):
            product = dot(table[...], tokens[h].reshape(width * samples, channels))
            send[:, h * row_chunk : (h + 1) * row_chunk, :] = product.astype(bf16).reshape(
                n, row_chunk, channels
            )

    columns(tok, col_tok, send_a)
    pl.semaphore_wait(barrier, n)
    move_a[0]()
    columns(cot, col_cot, send_b)
    move_b[0]()
    recv_a[me] = send_a[me]
    recv_b[me] = send_b[me]

    turn_back[...] = turn[...].T
    row_at = lax.broadcasted_iota(jnp.int32, (BLOCK, GROUP), 0)
    lane_at = lax.broadcasted_iota(jnp.int32, (BLOCK, GROUP), 1)
    for at, weight in enumerate((in_weight, out_weight)):
        for i in range(PER_GROUP):
            place = (lane_at == row_at + i * BLOCK).astype(bf16)
            for c in range(2):
                for g in range(groups):
                    wide[2 * at + c, g, i * BLOCK : (i + 1) * BLOCK, :] = dot(
                        weight[c, g * PER_GROUP + i], place
                    ).astype(bf16)

    half = turn.shape[0] // 2
    scale = math.sqrt(2.0 / math.pi)

    def lanes(g):
        return pl.ds(pl.multiple_of(g * GROUP, GROUP), GROUP)

    def per_group(act):
        def step(g, carry):
            act(g, lanes(g))
            return carry

        lax.fori_loop(0, groups, step, 0)

    def along_rows(recv, at, keep, g):
        keep[g] = dot(turn[...], recv[:, :, at].reshape(turn.shape[1], GROUP)).astype(bf16)

    def back_rows(send, at):
        send[:, :, at] = (
            dot(turn_back[...], mixed_modes[...]).astype(bf16).reshape(n, chunk, GROUP)
        )

    def forward_group(g, at):
        along_rows(recv_a, at, spec, g)
        re, im = spec[g, :half], spec[g, half:]
        w_re, w_im = wide[0, g], wide[1, g]
        for c in range(2):
            if c == 0:
                value = dot(re, w_re) - dot(im, w_im)
            else:
                value = dot(re, w_im) + dot(im, w_re)
            value = value + in_bias[c : c + 1, at]
            square = value * value
            tanh = jnp.tanh(scale * value * (1.0 + 0.044715 * square))
            hid[g, c * half : (c + 1) * half] = (0.5 * value * (1.0 + tanh)).astype(bf16)
            slope[g, c * half : (c + 1) * half] = 0.5 * (1.0 + tanh) + 0.5 * value * (
                1.0 - tanh * tanh
            ) * (scale * (1.0 + (3.0 * 0.044715) * square))
        re, im = hid[g, :half], hid[g, half:]
        w_re, w_im = wide[2, g], wide[3, g]
        mixed_modes[:half] = (
            dot(re, w_re) - dot(im, w_im) + out_bias[0:1, at]
        ).astype(bf16)
        mixed_modes[half:] = (
            dot(re, w_im) + dot(im, w_re) + out_bias[1:2, at]
        ).astype(bf16)
        back_rows(send_c, at)

    move_a[1]()
    per_group(forward_group)
    move_c[0]()
    recv_c[me] = send_c[me]

    def backward_group(g, at):
        along_rows(recv_b, at, inc, g)
        re, im = inc[g, :half], inc[g, half:]
        w_re, w_im = wide[2, g], wide[3, g]
        pre[g, :half] = (
            (dot(re, w_re, (1, 1)) + dot(im, w_im, (1, 1))) * slope[g, :half]
        ).astype(bf16)
        pre[g, half:] = (
            (dot(im, w_re, (1, 1)) - dot(re, w_im, (1, 1))) * slope[g, half:]
        ).astype(bf16)
        re, im = pre[g, :half], pre[g, half:]
        w_re, w_im = wide[0, g], wide[1, g]
        mixed_modes[:half] = (dot(re, w_re, (1, 1)) + dot(im, w_im, (1, 1))).astype(bf16)
        mixed_modes[half:] = (dot(im, w_re, (1, 1)) - dot(re, w_im, (1, 1))).astype(bf16)
        back_rows(send_d, at)

    move_b[1]()
    per_group(backward_group)

    def fold(product):
        total = jnp.zeros((BLOCK, GROUP), jnp.float32)
        for i in range(PER_GROUP):
            inside = (lane_at >= i * BLOCK) & (lane_at < (i + 1) * BLOCK)
            total = jnp.where(inside, product[i * BLOCK : (i + 1) * BLOCK], total)
        return total.astype(bf16)

    bias_at = lax.broadcasted_iota(jnp.int32, (16, GROUP), 0)

    def grads_group(g, at):
        bias = jnp.zeros((16, GROUP), jnp.float32)
        for k, (left, right) in enumerate(((spec, pre), (hid, inc))):
            a_re, a_im = left[g, :half], left[g, half:]
            b_re, b_im = right[g, :half], right[g, half:]
            first = 2 * k * BLOCK
            grads[first : first + BLOCK, at] = fold(
                dot(a_re, b_re, (0, 0)) + dot(a_im, b_im, (0, 0))
            )
            grads[first + BLOCK : first + 2 * BLOCK, at] = fold(
                dot(a_re, b_im, (0, 0)) - dot(a_im, b_re, (0, 0))
            )
            for c, value in enumerate((b_re, b_im)):
                total = jnp.sum(value.astype(jnp.float32), axis=0, keepdims=True)
                bias = jnp.where(bias_at == 2 * k + c, total, bias)
        grads[4 * BLOCK : 4 * BLOCK + 16, at] = bias.astype(bf16)

    per_group(grads_group)
    per = 4 * BLOCK // (2 * n)
    to_row = lax.broadcasted_iota(jnp.int32, (2 * n * 16, 4 * BLOCK + 16), 0)
    from_row = lax.broadcasted_iota(jnp.int32, (2 * n * 16, 4 * BLOCK + 16), 1)
    slot = to_row % 16
    wanted = jnp.where(slot < per, to_row // 16 * per + slot, 4 * BLOCK + slot - per)
    picks = (wanted == from_row).astype(bf16)
    halves[...] = dot(picks, grads[...]).astype(bf16).reshape(halves.shape)

    def swap(slot, source, target):
        return pltpu.make_async_remote_copy(
            src_ref=source,
            dst_ref=target,
            send_sem=pair_send.at[slot],
            recv_sem=pair_recv.at[slot],
            device_id={"rep": partner},
            device_id_type=MESH_ID,
        )

    first_swap = swap(0, halves.at[partner], half_in)
    first_swap.start()

    def inverse_row(h, tokens, table, recv, out):
        section = recv[:, h * row_chunk : (h + 1) * row_chunk, :]
        product = dot(table[...], section.reshape(n * row_chunk, channels))
        kept = tokens[h].reshape(width * samples, channels).astype(jnp.float32)
        out[h] = (kept + product).astype(bf16).reshape(width, samples, channels)

    def inverse(tokens, table, recv, out):
        for h in range(rows):
            inverse_row(h, tokens, table, recv, out)

    first_swap.wait()
    send_e[...] = (
        (halves[core].astype(jnp.float32) + half_in[...].astype(jnp.float32))
        .astype(bf16)
        .reshape(send_e.shape)
    )
    move_e[0]()
    recv_e[within] = send_e[within]
    pieces[0][0]()
    recv_d[me] = send_d[me]
    move_c[1]()
    inverse(tok, inv_mix, recv_c, mixed)

    move_e[1]()
    send_f[...] = jnp.sum(recv_e[...].astype(jnp.float32), axis=0).astype(bf16)
    move_f[0]()
    recv_f[across] = send_f[across]
    middle = max(2, rows - 1)
    for piece in pieces[1:middle]:
        piece[0]()
    move_f[1]()
    total = jnp.sum(recv_f[...].astype(jnp.float32), axis=0) * (1.0 / divisor)
    in_bias_grad[...] = total[per : per + 2]
    out_bias_grad[...] = total[per + 2 : per + 4]
    part[...] = total.astype(bf16)
    move_g[0]()
    gathered[within, across] = part[...]
    for piece in pieces[middle:]:
        piece[0]()
    pieces[0][1]()
    inverse_row(0, cot, inv_grad, recv_d, grad)
    move_g[1]()
    move_h[0]()
    for h in range(1, rows - 1):
        pieces[h][1]()
        inverse_row(h, cot, inv_grad, recv_d, grad)
    move_h[1]()
    last_swap = swap(1, gathered, other)
    last_swap.start()
    both[core] = gathered[...].reshape(n * 16, channels)
    for h in range(max(1, rows - 1), rows):
        pieces[h][1]()
        inverse_row(h, cot, inv_grad, recv_d, grad)
    last_swap.wait()
    both[partner] = other[...].reshape(n * 16, channels)
    to_row = lax.broadcasted_iota(jnp.int32, (2 * BLOCK, n * 16), 0)
    from_row = lax.broadcasted_iota(jnp.int32, (2 * BLOCK, n * 16), 1)
    order = (to_row // per * 16 + to_row % per == from_row).astype(bf16)
    for k, out in enumerate((in_weight_grad, out_weight_grad)):
        for g in range(groups):
            ordered = dot(order, both[k, :, g * GROUP : (g + 1) * GROUP]).astype(bf16)
            for i in range(PER_GROUP):
                place = (lane_at == row_at + i * BLOCK).astype(bf16)
                block = dot(ordered, place, (1, 1))
                for c in range(2):
                    out[c, g * PER_GROUP + i] = block[c * BLOCK : (c + 1) * BLOCK]

    for move in (move_a, move_b, move_c, move_e, move_f, move_g, move_h, *pieces):
        move[2]()


def fits(n, reps, samples, rows, channels):
    per_row = samples * (MODES // n) * 2
    return (
        reps == 2
        and MODES % n == 0
        and per_row % 16 == 0
        and channels % GROUP == 0
        and channels == BLOCKS * BLOCK
        and (4 * BLOCK) % (2 * n) == 0
        and n > 1
        and n & (n - 1) == 0
        and rows > 1
        and 4 * BLOCK // (2 * n) + 4 <= 16
        and (samples * MODES // n * rows * n) % 16 == 0
    )


def shards(tokens, cotangent, in_weight, in_bias, out_weight, out_bias):
    samples, rows, width, channels = tokens.shape
    n, reps = lax.axis_size("seq"), lax.axis_size("rep")
    if not fits(n, reps, samples, rows, channels):
        return shards_plain(tokens, cotangent, in_weight, in_bias, out_weight, out_bias)
    length = rows * n
    inner = 2 ** ((n.bit_length() - 1) // 2)
    outer = n // inner
    chunk = rows * samples * (MODES // n) * 2
    whole = n * chunk
    groups = channels // GROUP
    tables = [jnp.asarray(t) for t in kernel_tables(width, length, n, samples, rows)]
    bf16, f32 = jnp.bfloat16, jnp.float32
    block = pltpu.VMEM((n, chunk, channels), bf16)
    small = pltpu.VMEM((n, 16, channels), bf16)
    ringed = pltpu.VMEM((inner, outer, 16, channels), bf16)
    lined = pltpu.VMEM((outer, 16, channels), bf16)
    planes = (tokens.transpose(1, 2, 0, 3), cotangent.transpose(1, 2, 0, 3))
    kept = pltpu.VMEM((groups, whole, GROUP), bf16)
    vmem = pl.BlockSpec(memory_space=pltpu.VMEM)
    mixed, grad, *parameter_grads = pl.pallas_call(
        functools.partial(mixer, n, inner, float(samples * reps)),
        out_shape=(
            jax.ShapeDtypeStruct(planes[0].shape, bf16),
            jax.ShapeDtypeStruct(planes[1].shape, bf16),
            jax.ShapeDtypeStruct(in_weight.shape, f32),
            jax.ShapeDtypeStruct(in_bias.shape, f32),
            jax.ShapeDtypeStruct(out_weight.shape, f32),
            jax.ShapeDtypeStruct(out_bias.shape, f32),
        ),
        in_specs=[vmem] * 11,
        out_specs=(vmem,) * 6,
        scratch_shapes=[block] * 4
        + [ringed, lined]
        + [block] * 4
        + [ringed, lined]
        + [
            pltpu.VMEM((whole, whole), bf16),
            pltpu.VMEM((4, groups, GROUP, GROUP), bf16),
            kept,
            kept,
            pltpu.VMEM((groups, whole, GROUP), f32),
            kept,
            kept,
            pltpu.VMEM((whole, GROUP), bf16),
            pltpu.VMEM((4 * BLOCK + 16, channels), bf16),
            pltpu.VMEM((2, n, 16, channels), bf16),
            small,
            pltpu.VMEM((16, channels), bf16),
            ringed,
            ringed,
            pltpu.VMEM((2, n * 16, channels), bf16),
            pltpu.SemaphoreType.DMA((COPY_D + rows, n)),
            pltpu.SemaphoreType.DMA((COPY_D + rows, n)),
            pltpu.SemaphoreType.DMA((2,)),
            pltpu.SemaphoreType.DMA((2,)),
        ],
        compiler_params=pltpu.CompilerParams(
            collective_id=0, has_side_effects=True, vmem_limit_bytes=63 << 20
        ),
        name="mixer",
    )(*planes, *tables, in_weight, in_bias, out_weight, out_bias)
    return (
        mixed.transpose(2, 0, 1, 3),
        grad.transpose(2, 0, 1, 3),
        *parameter_grads,
    )


def solution(mesh):
    in_specs = (P("rep", "seq", None, None), P("rep", "seq", None, None), P(), P(), P(), P())
    out_specs = (P("rep", "seq", None, None), P("rep", "seq", None, None), P(), P(), P(), P())
    return jax.shard_map(shards, mesh=mesh, in_specs=in_specs, out_specs=out_specs, check_vma=False)
```
